512 devices in a mesh: rows: 128 (over x_hi, z, y), feat: 4 (over x_lo, core).
Axes of the slice: x: 4 (x_hi: 2, x_lo: 2; x = x_hi * 2 + x_lo), y: 8, z: 8, core: 2. Of those that a mesh axis runs over, the one named last changes fastest.
Arguments:
- features: bfloat16 [131072, 64], P('rows', 'feat'), may hold values from -0.75 to 0.75
- probes: bfloat16 [131072, 32], P('rows', 'feat'), may hold values from -6 to 6
- theta: float32 [1], replicated, may hold values from 0.18 to 0.69
- block_mask: int32 [128, 9], P('rows'), may hold values 0 or 1
- order: int32 [128, 1024], P('rows'), may hold values from 0 to 1023, each once within a row
Outputs:
- kernel_probes: float32 [131072, 32], P('rows', 'feat')
- deriv_probes: float32 [131072, 32], P('rows', 'feat')
The draws below stay inside these ranges and needn't reach their ends.
All inputs are finite; a program needn't handle non-finite values. No bound on the sum of `block_mask` on one device may be relied on, other than what follows from the above.
Results may differ from the reference program's by a relative error of at most 0.003.
Values may be sent and summed in bfloat16 or wider, within the bound.
A program may use at most 64 MiB of HBM per device.

```python
import jax
import jax.numpy as jnp
from jax import lax

F = 64
P_SIZE = 32
ROWS_DEV = 1024
NBLK = 128
N = 131072


def touch_ends(entries, rng, smallest, top_value):
    longest = entries.shape.index(max(entries.shape))
    spots = []
    for shift in (0, 1):
        where = [jax.random.randint(jax.random.fold_in(rng, axis), (), 0, length) for axis, length in enumerate(entries.shape)]
        where[longest] = (where[longest] + shift) % entries.shape[longest]
        spots.append(tuple(where))
    return entries.at[spots[0]].set(smallest).at[spots[1]].set(top_value)


def levels(rng, dims, cuts, low, largest):
    def one(position, shards_of):
        heights = jax.random.uniform(jax.random.fold_in(jax.random.fold_in(rng, 6), position), (shards_of,), jnp.float32, low / len(cuts), largest / len(cuts))
        return jnp.repeat(jnp.exp(heights), dims[position] // shards_of).reshape((-1,) + (1,) * (len(dims) - position - 1))

    factor_of = one(*cuts[0])
    for cut in cuts[1:]:
        factor_of = factor_of * one(*cut)
    return factor_of


def gaussian(stream_key, extent, deviation, most, pieces=(), held_as=jnp.bfloat16):
    entries = deviation * jax.random.normal(stream_key, extent, jnp.float32)
    if pieces:
        entries = entries * levels(stream_key, extent, pieces, -0.22, 0.18)
    return jnp.clip(entries, -most, most).astype(held_as)


def setup_inputs(seed: int = 0) -> dict:
    streams_of = jax.random.split(jax.random.key(seed), 6)
    features = gaussian(streams_of[0], (N, F), (1.0 / F ** 0.5), 0.75, ((0, 128), (1, 4)))
    probes = gaussian(streams_of[1], (N, P_SIZE), 1.0, 6.0, ((0, 128), (1, 4)))
    theta = jnp.clip(jax.random.uniform(streams_of[2], (1,), jnp.float32, 0.18, 0.69), 0.18, 0.69)
    block_mask = touch_ends((jax.random.randint(streams_of[3], (NBLK, 9), 0, 4) < 3).astype(jnp.int32), jax.random.fold_in(streams_of[3], 1), 0, 1)
    order = jax.vmap(lambda own: jax.random.permutation(own, ROWS_DEV))(jax.random.split(streams_of[4], NBLK)).reshape((NBLK, ROWS_DEV)).astype(jnp.int32)
    return {"features": features, "probes": probes, "theta": theta, "block_mask": block_mask, "order": order}


def reference(features, probes, theta, block_mask, order):
    feats = features.reshape(NBLK, ROWS_DEV, F)
    raw = probes.reshape(NBLK, ROWS_DEV, P_SIZE)
    ordered = jnp.take_along_axis(raw, order.astype(jnp.int32)[:, :, None], axis=1)
    squares = lax.optimization_barrier(jnp.sum(feats.astype(jnp.float32) ** 2, axis=2))
    scale = jnp.exp(-2.0 * theta[0])

    def one_block(index):
        rows_f = lax.dynamic_index_in_dim(feats, index, 0, keepdims=False)
        rows_sq = lax.dynamic_index_in_dim(squares, index, 0, keepdims=False)
        total_k = jnp.zeros((ROWS_DEV, P_SIZE), jnp.float32)
        total_d = jnp.zeros((ROWS_DEV, P_SIZE), jnp.float32)
        for offset in range(9):
            other = ((index + offset - 4) % NBLK).astype(jnp.int32)
            cols_f = lax.dynamic_index_in_dim(feats, other, 0, keepdims=False)
            cols_sq = lax.dynamic_index_in_dim(squares, other, 0, keepdims=False)
            cols_z = lax.dynamic_index_in_dim(ordered, other, 0, keepdims=False)
            cross = lax.dot_general(rows_f, cols_f, (((1,), (1,)), ((), ())), preferred_element_type=jnp.float32)
            dist2 = jnp.maximum(rows_sq[:, None] + cols_sq[None, :] - 2.0 * cross, 0.0)
            radius2 = dist2 * scale
            radius = jnp.sqrt(radius2)
            inside = jnp.maximum(1.0 - radius, 0.0)
            inside2 = inside * inside
            kern = (inside2 * inside2 * (4.0 * radius + 1.0)).astype(jnp.bfloat16)
            deriv = (20.0 * radius2 * inside2 * inside).astype(jnp.bfloat16)
            term_k = jnp.dot(kern, cols_z, preferred_element_type=jnp.float32)
            term_d = jnp.dot(deriv, cols_z, preferred_element_type=jnp.float32)
            if offset == 4:
                total_k = total_k + term_k
                total_d = total_d + term_d
            else:
                active = block_mask[index, offset] > 0
                total_k = total_k + jnp.where(active, term_k, 0.0)
                total_d = total_d + jnp.where(active, term_d, 0.0)
        return (total_k, total_d)
    out_k, out_d = lax.map(one_block, jnp.arange(NBLK, dtype=jnp.int32))
    return (out_k.reshape(N, P_SIZE), out_d.reshape(N, P_SIZE))
```

```python
import functools

import jax
import jax.numpy as jnp
from jax import lax
from jax.experimental import pallas as pl
from jax.experimental.pallas import tpu as pltpu
from jax.sharding import PartitionSpec as P

MESH = pl.DeviceIdType.MESH
BF = jnp.bfloat16
F32 = jnp.float32
ROUTE = {1: 1, 2: 2, 3: 1, 4: 2}
OFFS = (1, -1, 2, -2, 3, -3, 4, -4)
SLOT = {k: i for i, k in enumerate(OFFS)}
DIRECT = [k for k in OFFS if ROUTE[abs(k)] == abs(k)]
TINY = 1e-30


def rounded(value):
    return value.astype(BF).astype(F32)


def split3(value):
    high = rounded(value)
    rest = value - high
    middle = rounded(rest)
    return high, middle, rest - middle


def stacked_rows(rows, width):
    index = lax.broadcasted_iota(jnp.int32, (8, width), 0)
    out = jnp.zeros((8, width), F32)
    for place, row in enumerate(rows):
        out = jnp.where(index == place, row, out)
    return out


def kernel(
    blocks, feats, ft, pt, theta, mask, order, out_k, out_d,
    own, raw, order_v, full, own_z, slots, right, acc_k, acc_d, out_s, out_r,
    load_sem, full_send, full_recv, z_send, z_recv, slot_send, slot_recv, red_send, red_recv,
):
    row = lax.axis_index("rows")
    col = lax.axis_index("feat")
    points = own.shape[2]
    panel = points // feats
    width = panel

    def at(step):
        return lax.rem(row + step + blocks, blocks)

    def device(step, other):
        return (at(step), other)

    def peer(i):
        return lax.rem(col + i, feats)

    barrier = pltpu.get_barrier_semaphore()
    greeted = 0
    for i in range(1, feats):
        pl.semaphore_signal(barrier, inc=1, device_id=(row, peer(i)), device_id_type=MESH)
        greeted += 1
    reach = sorted({s * ROUTE[abs(k)] for k in OFFS for s in (1, -1)}, key=abs)
    for step in reach:
        for other in range(feats):
            pl.semaphore_signal(barrier, inc=1, device_id=device(step, other), device_id_type=MESH)
            greeted += 1

    loads = [
        pltpu.make_async_copy(order, order_v, load_sem.at[0]),
        pltpu.make_async_copy(pt, raw, load_sem.at[1]),
        pltpu.make_async_copy(ft, own.at[0:2], load_sem.at[2]),
        pltpu.make_async_copy(ft, full.at[col], load_sem.at[3]),
    ]
    for load in loads:
        load.start()

    scale16 = 16.0 * jnp.exp(jnp.full((1, panel), -2.0 * theta[0], F32))

    loads[0].wait()
    loads[1].wait()
    wanted = order_v[...]
    ordered = jnp.zeros((8, points), F32)
    for part in range(points // panel):
        source = lax.broadcasted_iota(jnp.int32, (panel, points), 0) + part * panel
        chosen = jnp.where(source == wanted, 1.0, 0.0).astype(BF)
        ordered = ordered + jnp.dot(
            raw[:, part * panel : (part + 1) * panel], chosen, preferred_element_type=F32
        )
    own[2] = ordered.astype(BF)
    loads[2].wait()
    loads[3].wait()
    mine = pl.ds(pl.multiple_of(col * panel, panel), panel)
    own_z[col] = own[2, :, mine]

    pl.semaphore_wait(barrier, greeted)

    sent = []

    def send_direct(k):
        for i in range(feats):
            other = peer(i)
            copy = pltpu.make_async_remote_copy(
                src_ref=own.at[:, :, pl.ds(pl.multiple_of(other * panel, panel), panel)],
                dst_ref=slots.at[SLOT[k], col],
                send_sem=slot_send.at[SLOT[k], i],
                recv_sem=slot_recv.at[SLOT[k], col],
                device_id=device(-k, other),
                device_id_type=MESH,
            )
            copy.start()
            sent.append(copy)

    far_first = sorted(DIRECT, key=lambda k: -abs(k))
    for k in far_first:
        send_direct(k)
    for i in range(1, feats):
        other = peer(i)
        copy = pltpu.make_async_remote_copy(
            src_ref=own.at[0:2],
            dst_ref=full.at[col],
            send_sem=full_send.at[i],
            recv_sem=full_recv.at[col],
            device_id=(row, other),
            device_id_type=MESH,
        )
        copy.start()
        sent.append(copy)
        copy = pltpu.make_async_remote_copy(
            src_ref=own.at[2, :, pl.ds(pl.multiple_of(other * panel, panel), panel)],
            dst_ref=own_z.at[col],
            send_sem=z_send.at[i],
            recv_sem=z_recv.at[col],
            device_id=(row, other),
            device_id_type=MESH,
        )
        copy.start()
        sent.append(copy)

    def arrival(k, source):
        return pltpu.make_async_remote_copy(
            src_ref=slots.at[SLOT[k], source],
            dst_ref=slots.at[SLOT[k], source],
            send_sem=slot_send.at[SLOT[k], 0],
            recv_sem=slot_recv.at[SLOT[k], source],
            device_id=(row, peer(1)),
            device_id_type=MESH,
        )

    def wait_and_forward(k):
        for i in range(feats):
            source = peer(i)
            arrival(k, source).wait_recv()
            for further in OFFS:
                by = ROUTE[abs(further)]
                if by == abs(further) or further * k < 0 or abs(further) - by != abs(k):
                    continue
                step = by if k > 0 else -by
                copy = pltpu.make_async_remote_copy(
                    src_ref=slots.at[SLOT[k], source],
                    dst_ref=slots.at[SLOT[further], source],
                    send_sem=slot_send.at[SLOT[further], i],
                    recv_sem=slot_recv.at[SLOT[further], source],
                    device_id=device(-step, col),
                    device_id_type=MESH,
                )
                copy.start()
                sent.append(copy)

    def panel_left(feature_rows):
        squares = jnp.sum(feature_rows * feature_rows, axis=0, keepdims=True) * scale16
        packed = feature_rows.astype(BF)
        one = jnp.ones((1, panel), F32)
        extra = stacked_rows([*split3(squares), one, one, one], panel)
        extra = jnp.concatenate([extra, jnp.zeros((56, panel), F32)], axis=0).astype(BF)
        flat = jnp.concatenate([packed, packed, packed, extra], axis=0)
        return flat.T

    acc_k[...] = jnp.zeros_like(acc_k)
    acc_d[...] = jnp.zeros_like(acc_d)

    def tile(left, z, c):
        lanes = pl.ds(c * width, width)
        x = jnp.dot(left, right[:, lanes], preferred_element_type=F32)
        x = jnp.maximum(x, TINY)
        r = x * lax.rsqrt(x)
        u = jnp.maximum(4.0 - r, 0.0)
        u3 = u * u * u
        kern = (u3 * (u * (r + 1.0))).astype(BF)
        deriv = (u3 * (1.25 * x)).astype(BF)
        return (
            jnp.dot(z, kern, preferred_element_type=F32),
            jnp.dot(z, deriv, preferred_element_type=F32),
        )

    def slot_operands(k):
        values = slots[SLOT[k]].astype(F32)
        features = values[:, 0:2].reshape(64, panel)
        active = jnp.where(mask[0, 4 + k] > 0, 1.0, 0.0)
        z = (values[:, 2].reshape(32, panel) * active).astype(BF)
        return panel_left(features), z

    relays = [k for k in OFFS if any(abs(f) - ROUTE[abs(f)] == abs(k) for f in OFFS)]
    for k in relays:
        wait_and_forward(k)

    for i in range(1, feats):
        source = peer(i)
        pltpu.make_async_remote_copy(
            src_ref=own.at[0:2], dst_ref=full.at[source], send_sem=full_send.at[i],
            recv_sem=full_recv.at[source], device_id=(row, source), device_id_type=MESH,
        ).wait_recv()
        pltpu.make_async_remote_copy(
            src_ref=own_z.at[source], dst_ref=own_z.at[source], send_sem=z_send.at[i],
            recv_sem=z_recv.at[source], device_id=(row, source), device_id_type=MESH,
        ).wait_recv()

    for c in range(points // width):
        lanes = slice(c * width, (c + 1) * width)
        f = full[:, :, :, lanes].astype(F32).reshape(64, width)
        squares = jnp.sum(f * f, axis=0, keepdims=True) * scale16
        one = jnp.ones((1, width), F32)
        extra = stacked_rows([one, one, one, *split3(squares)], width)
        extra = jnp.concatenate([extra, jnp.zeros((56, width), F32)], axis=0)
        high, middle, low = split3(f * (-2.0 * scale16))
        right[:, lanes] = jnp.concatenate([high, middle, low, extra], axis=0).astype(BF)

    def accumulate(pairs):
        for c in range(points // width):
            lanes = pl.ds(c * width, width)
            total_k, total_d = acc_k[:, lanes], acc_d[:, lanes]
            for left, z in pairs:
                add_k, add_d = tile(left, z, c)
                total_k, total_d = total_k + add_k, total_d + add_d
            acc_k[:, lanes], acc_d[:, lanes] = total_k, total_d

    own_features = full[:, :, :, mine].astype(F32).reshape(64, panel)
    own_probes = own_z[...].astype(F32).reshape(32, panel).astype(BF)
    accumulate([(panel_left(own_features), own_probes)])

    waited = set(relays)
    for k in (1, 2, 3):
        for s in (k, -k):
            if s not in waited:
                wait_and_forward(s)
        accumulate([slot_operands(k), slot_operands(-k)])
    for s in (4, -4):
        wait_and_forward(s)
    last = [slot_operands(4), slot_operands(-4)]
    for c in range(points // width):
        lanes = pl.ds(c * width, width)
        total_k, total_d = acc_k[:, lanes], acc_d[:, lanes]
        for left, z in last:
            add_k, add_d = tile(left, z, c)
            total_k, total_d = total_k + add_k, total_d + add_d
        total_k, total_d = total_k * (1.0 / 256.0), total_d * (1.0 / 64.0)
        acc_k[:, lanes], acc_d[:, lanes] = total_k, total_d
        out_s[c, :, 0] = total_k.astype(BF).reshape(feats, 8, width)
        out_s[c, :, 1] = total_d.astype(BF).reshape(feats, 8, width)
        for i in range(1, feats):
            other = peer(i)
            copy = pltpu.make_async_remote_copy(
                src_ref=out_s.at[c, other],
                dst_ref=out_r.at[c, col],
                send_sem=red_send.at[c, i],
                recv_sem=red_recv.at[c, col],
                device_id=(row, other),
                device_id_type=MESH,
            )
            copy.start()
            sent.append(copy)

    probes_here = pl.ds(pl.multiple_of(col * 8, 8), 8)
    for c in range(points // width):
        lanes = pl.ds(c * width, width)
        total_k, total_d = acc_k[probes_here, lanes], acc_d[probes_here, lanes]
        for i in range(1, feats):
            source = peer(i)
            pltpu.make_async_remote_copy(
                src_ref=out_s.at[c, source], dst_ref=out_r.at[c, source], send_sem=red_send.at[c, i],
                recv_sem=red_recv.at[c, source], device_id=(row, source), device_id_type=MESH,
            ).wait_recv()
            total_k = total_k + out_r[c, source, 0].astype(F32)
            total_d = total_d + out_r[c, source, 1].astype(F32)
        out_k[:, lanes], out_d[:, lanes] = total_k, total_d

    for copy in sent:
        copy.wait_send()


def solution(mesh):
    blocks, feats = mesh.shape["rows"], mesh.shape["feat"]

    def body(features, probes, theta, block_mask, order):
        points, width = features.shape
        columns = probes.shape[1]
        panel = points // feats
        chunks = feats
        ft = features.T.reshape(2, width // 2, points)
        pt = probes.T
        any_space = pl.BlockSpec(memory_space=pl.ANY)
        small = pl.BlockSpec(memory_space=pltpu.SMEM)
        vmem = pl.BlockSpec(memory_space=pltpu.VMEM)
        dma = pltpu.SemaphoreType.DMA
        out = jax.ShapeDtypeStruct((columns, points), F32)
        out_k, out_d = pl.pallas_call(
            functools.partial(kernel, blocks, feats),
            out_shape=(out, out),
            in_specs=[any_space, any_space, small, small, any_space],
            out_specs=(vmem, vmem),
            scratch_shapes=[
                pltpu.VMEM((3, 8, points), BF),
                pltpu.VMEM((8, points), BF),
                pltpu.VMEM((1, points), jnp.int32),
                pltpu.VMEM((feats, 2, 8, points), BF),
                pltpu.VMEM((feats, 8, panel), BF),
                pltpu.VMEM((8, feats, 3, 8, panel), BF),
                pltpu.VMEM((256, points), BF),
                pltpu.VMEM((feats * columns, points), F32),
                pltpu.VMEM((feats * columns, points), F32),
                pltpu.VMEM((chunks, feats, 2, 8, points // chunks), BF),
                pltpu.VMEM((chunks, feats, 2, 8, points // chunks), BF),
                dma((4,)),
                dma((feats,)), dma((feats,)), dma((feats,)), dma((feats,)),
                dma((8, feats)), dma((8, feats)),
                dma((chunks, feats)), dma((chunks, feats)),
            ],
            compiler_params=pltpu.CompilerParams(collective_id=0, has_side_effects=True),
        )(ft, pt, theta, block_mask, order)
        return out_k.T, out_d.T

    return jax.shard_map(
        body,
        mesh=mesh,
        in_specs=(P("rows", "feat"), P("rows", "feat"), P(), P("rows", None), P("rows", None)),
        out_specs=(P("rows", "feat"), P("rows", "feat")),
        check_vma=False,
    )
```

```python
import functools

import jax
import jax.numpy as jnp
from jax import lax
from jax.experimental import pallas as pl
from jax.experimental.pallas import tpu as pltpu
from jax.sharding import PartitionSpec as P

MESH = pl.DeviceIdType.MESH
BF = jnp.bfloat16
F32 = jnp.float32
OFFS = (1, -1, 2, -2, 3, -3, 4, -4)
SLOT = {k: i for i, k in enumerate(OFFS)}
TINY = 1e-30
FAR = ((0, -2), (0, -3), (0, -4), (2, -3), (2, -4))


def rounded(value):
    return value.astype(BF).astype(F32)


def split3(value):
    high = rounded(value)
    rest = value - high
    middle = rounded(rest)
    return high, middle, rest - middle


def stacked_rows(rows, width):
    index = lax.broadcasted_iota(jnp.int32, (8, width), 0)
    out = jnp.zeros((8, width), F32)
    for place, row in enumerate(rows):
        out = jnp.where(index == place, row, out)
    return out


def kernel(
    blocks, feats, ft, pt, theta, mask_in, order, out_k, out_d,
    mask, own, raw, order_v, full, own_z, slots, right, acc_k, acc_d, out_s, out_r,
    late_in, load_sem, full_send, full_recv, z_send, z_recv, far_sem, slot_send, slot_recv, red_send, red_recv,
):
    row = lax.axis_index("rows")
    col = lax.axis_index("feat")
    points = own.shape[2]
    panel = points // feats
    width = panel

    def at(step):
        return lax.rem(row + step + blocks, blocks)

    def device(step, other):
        return (at(step), other)

    def peer(i):
        return lax.rem(col + i, feats)

    loads = [
        pltpu.make_async_copy(order, order_v, load_sem.at[0]),
        pltpu.make_async_copy(pt, raw, load_sem.at[1]),
        pltpu.make_async_copy(ft, own.at[0:2], load_sem.at[2]),
        pltpu.make_async_copy(ft, full.at[col], load_sem.at[3]),
        pltpu.make_async_copy(mask_in, mask, load_sem.at[4]),
    ]
    for load in loads:
        load.start()

    half = blocks // 2
    place = lax.rem(row, half)
    lowest, highest = place == 0, place == half - 1

    barrier = pltpu.get_barrier_semaphore()

    def greet(target):
        pl.semaphore_signal(barrier, inc=1, device_id=target, device_id_type=MESH)

    def greet_block(step):
        for other in range(feats):
            greet(device(step, other))

    for i in range(1, feats):
        greet((row, peer(i)))
    greet_block(-1)
    pl.when(jnp.logical_not(highest))(lambda: greet_block(1))
    for target, k in FAR:
        pl.when(place == target)(functools.partial(greet_block, k))

    def count(condition):
        return condition.astype(jnp.int32)

    greeted = (feats - 1) + feats + feats * count(place != 0)
    for target, k in FAR:
        greeted = greeted + feats * count(place == half + target + k)

    loads[0].wait()
    loads[1].wait()
    wanted = order_v[...]
    ordered = jnp.zeros((8, points), F32)
    for part in range(points // panel):
        source = lax.broadcasted_iota(jnp.int32, (panel, points), 0) + part * panel
        chosen = jnp.where(source == wanted, 1.0, 0.0).astype(BF)
        ordered = ordered + jnp.dot(
            raw[:, part * panel : (part + 1) * panel], chosen, preferred_element_type=F32
        )
    own[2] = ordered.astype(BF)
    for load in loads[2:]:
        load.wait()
    scale16 = 16.0 * jnp.exp(jnp.full((1, panel), -2.0 * theta[0], F32))
    mine = pl.ds(pl.multiple_of(col * panel, panel), panel)
    own_z[col] = own[2, :, mine]

    pl.semaphore_wait(barrier, greeted)

    @pl.when(highest)
    def _():
        for other in range(feats):
            pl.semaphore_signal(late_in, inc=1, device_id=device(1, other), device_id_type=MESH)

    sent = []

    def direct(k, i):
        other = peer(i)
        return pltpu.make_async_remote_copy(
            src_ref=own.at[:, :, pl.ds(pl.multiple_of(other * panel, panel), panel)],
            dst_ref=slots.at[SLOT[k], col],
            send_sem=slot_send.at[SLOT[k], i],
            recv_sem=slot_recv.at[SLOT[k], col],
            device_id=device(-k, other),
            device_id_type=MESH,
        )

    def forward(k, i):
        source = peer(i)
        step = 1 if k > 0 else -1
        return pltpu.make_async_remote_copy(
            src_ref=slots.at[SLOT[k - step], source],
            dst_ref=slots.at[SLOT[k], source],
            send_sem=slot_send.at[SLOT[k], i],
            recv_sem=slot_recv.at[SLOT[k], source],
            device_id=device(-step, col),
            device_id_type=MESH,
        )

    def far_send(target, k, i):
        other = peer(i)
        return pltpu.make_async_remote_copy(
            src_ref=own.at[:, :, pl.ds(pl.multiple_of(other * panel, panel), panel)],
            dst_ref=slots.at[SLOT[k], col],
            send_sem=far_sem.at[target // 2, i],
            recv_sem=slot_recv.at[SLOT[k], col],
            device_id=device(-k, other),
            device_id_type=MESH,
        )

    def start_all(make, *which):
        for i in range(feats):
            make(*which, i).start()

    def wait_all(make, *which):
        for i in range(feats):
            make(*which, i).wait_send()

    def forwarded(k):
        if k > 0:
            return place != 0
        far = [half - 1] + [target - 1 for target, slot in FAR if slot == k and target > 0]
        yes = place != far[0]
        for other in far[1:]:
            yes = yes & (place != other)
        return yes

    start_all(direct, -1)
    for target, k in FAR:
        pl.when(place == half + target + k)(functools.partial(start_all, far_send, target, k))
    pl.when(jnp.logical_not(lowest))(functools.partial(start_all, direct, 1))
    for i in range(1, feats):
        other = peer(i)
        copy = pltpu.make_async_remote_copy(
            src_ref=own.at[0:2],
            dst_ref=full.at[col],
            send_sem=full_send.at[i],
            recv_sem=full_recv.at[col],
            device_id=(row, other),
            device_id_type=MESH,
        )
        copy.start()
        sent.append(copy)
        copy = pltpu.make_async_remote_copy(
            src_ref=own.at[2, :, pl.ds(pl.multiple_of(other * panel, panel), panel)],
            dst_ref=own_z.at[col],
            send_sem=z_send.at[i],
            recv_sem=z_recv.at[col],
            device_id=(row, other),
            device_id_type=MESH,
        )
        copy.start()
        sent.append(copy)

    def arrival(k, source):
        return pltpu.make_async_remote_copy(
            src_ref=slots.at[SLOT[k], source],
            dst_ref=slots.at[SLOT[k], source],
            send_sem=slot_send.at[SLOT[k], 0],
            recv_sem=slot_recv.at[SLOT[k], source],
            device_id=(row, peer(1)),
            device_id_type=MESH,
        )

    def wait_and_forward(k):
        further = k + (1 if k > 0 else -1)
        for i in range(feats):
            arrival(k, peer(i)).wait_recv()
            if abs(further) <= 4:
                pl.when(forwarded(further))(forward(further, i).start)

    def panel_left(feature_rows):
        squares = jnp.sum(feature_rows * feature_rows, axis=0, keepdims=True) * scale16
        packed = feature_rows.astype(BF)
        one = jnp.ones((1, panel), F32)
        extra = stacked_rows([*split3(squares), one, one, one], panel)
        extra = jnp.concatenate([extra, jnp.zeros((56, panel), F32)], axis=0).astype(BF)
        flat = jnp.concatenate([packed, packed, packed, extra], axis=0)
        return flat.T

    acc_k[...] = jnp.zeros_like(acc_k)
    acc_d[...] = jnp.zeros_like(acc_d)

    def tile(left, z, c):
        lanes = pl.ds(c * width, width)
        x = jnp.dot(left, right[:, lanes], preferred_element_type=F32)
        x = jnp.maximum(x, TINY)
        r = x * lax.rsqrt(x)
        u = jnp.maximum(4.0 - r, 0.0)
        u3 = u * u * u
        kern = (u3 * (u * (r + 1.0))).astype(BF)
        deriv = (u3 * (1.25 * x)).astype(BF)
        return (
            jnp.dot(z, kern, preferred_element_type=F32),
            jnp.dot(z, deriv, preferred_element_type=F32),
        )

    def slot_operands(k):
        values = slots[SLOT[k]].astype(F32)
        features = values[:, 0:2].reshape(64, panel)
        active = jnp.where(mask[0, 4 + k] > 0, 1.0, 0.0)
        z = (values[:, 2].reshape(32, panel) * active).astype(BF)
        return panel_left(features), z

    def take(k):
        wait_and_forward(k)

        @pl.when(place >= k)
        def _():
            wait_and_forward(-k)

    take(1)
    for i in range(1, feats):
        source = peer(i)
        pltpu.make_async_remote_copy(
            src_ref=own.at[0:2], dst_ref=full.at[source], send_sem=full_send.at[i],
            recv_sem=full_recv.at[source], device_id=(row, source), device_id_type=MESH,
        ).wait_recv()
        pltpu.make_async_remote_copy(
            src_ref=own_z.at[source], dst_ref=own_z.at[source], send_sem=z_send.at[i],
            recv_sem=z_recv.at[source], device_id=(row, source), device_id_type=MESH,
        ).wait_recv()

    for c in range(points // width):
        lanes = slice(c * width, (c + 1) * width)
        f = full[:, :, :, lanes].astype(F32).reshape(64, width)
        squares = jnp.sum(f * f, axis=0, keepdims=True) * scale16
        one = jnp.ones((1, width), F32)
        extra = stacked_rows([one, one, one, *split3(squares)], width)
        extra = jnp.concatenate([extra, jnp.zeros((56, width), F32)], axis=0)
        high, middle, low = split3(f * (-2.0 * scale16))
        right[:, lanes] = jnp.concatenate([high, middle, low, extra], axis=0).astype(BF)

    def accumulate(pairs):
        for c in range(points // width):
            lanes = pl.ds(c * width, width)
            total_k, total_d = acc_k[:, lanes], acc_d[:, lanes]
            for left, z in pairs:
                add_k, add_d = tile(left, z, c)
                total_k, total_d = total_k + add_k, total_d + add_d
            acc_k[:, lanes], acc_d[:, lanes] = total_k, total_d

    own_features = full[:, :, :, mine].astype(F32).reshape(64, panel)
    own_probes = own_z[...].astype(F32).reshape(32, panel).astype(BF)
    accumulate([(panel_left(own_features), own_probes)])

    accumulate([slot_operands(1)])
    for k in (2, 3, 4):
        take(k)
        accumulate([slot_operands(k)])

    @pl.when(lowest)
    def _():
        pl.semaphore_wait(late_in, feats)
        start_all(direct, 1)
        for k in (2, 3, 4):
            start_all(forward, k)

    for k in (-1, -2, -3, -4):
        @pl.when(place < -k)
        def _():
            wait_and_forward(k)

        if k > -4:
            accumulate([slot_operands(k)])
    last = [slot_operands(-4)]
    for c in range(points // width):
        lanes = pl.ds(c * width, width)
        total_k, total_d = acc_k[:, lanes], acc_d[:, lanes]
        for left, z in last:
            add_k, add_d = tile(left, z, c)
            total_k, total_d = total_k + add_k, total_d + add_d
        total_k, total_d = total_k * (1.0 / 256.0), total_d * (1.0 / 64.0)
        acc_k[:, lanes], acc_d[:, lanes] = total_k, total_d
        out_s[c, :, 0] = total_k.astype(BF).reshape(feats, 8, width)
        out_s[c, :, 1] = total_d.astype(BF).reshape(feats, 8, width)
        for i in range(1, feats):
            other = peer(i)
            copy = pltpu.make_async_remote_copy(
                src_ref=out_s.at[c, other],
                dst_ref=out_r.at[c, col],
                send_sem=red_send.at[c, i],
                recv_sem=red_recv.at[c, col],
                device_id=(row, other),
                device_id_type=MESH,
            )
            copy.start()
            sent.append(copy)

    probes_here = pl.ds(pl.multiple_of(col * 8, 8), 8)
    for c in range(points // width):
        lanes = pl.ds(c * width, width)
        total_k, total_d = acc_k[probes_here, lanes], acc_d[probes_here, lanes]
        for i in range(1, feats):
            source = peer(i)
            pltpu.make_async_remote_copy(
                src_ref=out_s.at[c, source], dst_ref=out_r.at[c, source], send_sem=red_send.at[c, i],
                recv_sem=red_recv.at[c, source], device_id=(row, source), device_id_type=MESH,
            ).wait_recv()
            total_k = total_k + out_r[c, source, 0].astype(F32)
            total_d = total_d + out_r[c, source, 1].astype(F32)
        out_k[:, lanes], out_d[:, lanes] = total_k, total_d

    for copy in sent:
        copy.wait_send()
    for k in (1, -1):
        wait_all(direct, k)
    for k in (2, 3, 4):
        wait_all(forward, k)
        pl.when(forwarded(-k))(functools.partial(wait_all, forward, -k))
    for target, k in FAR:
        pl.when(place == half + target + k)(functools.partial(wait_all, far_send, target, k))


def solution(mesh):
    blocks, feats = mesh.shape["rows"], mesh.shape["feat"]

    def body(features, probes, theta, block_mask, order):
        points, width = features.shape
        columns = probes.shape[1]
        panel = points // feats
        chunks = feats
        ft = features.T.reshape(2, width // 2, points)
        pt = probes.T
        hbm = pl.BlockSpec(memory_space=pltpu.HBM)
        small = pl.BlockSpec(memory_space=pltpu.SMEM)
        placed = functools.partial(pltpu.with_memory_space_constraint, memory_space=pltpu.HBM)
        vmem = pl.BlockSpec(memory_space=pltpu.VMEM)
        dma = pltpu.SemaphoreType.DMA
        out = jax.ShapeDtypeStruct((columns, points), F32)
        out_k, out_d = pl.pallas_call(
            functools.partial(kernel, blocks, feats),
            out_shape=(out, out),
            in_specs=[hbm, hbm, small, hbm, hbm],
            out_specs=(vmem, vmem),
            scratch_shapes=[
                pltpu.SMEM((1, block_mask.shape[1]), jnp.int32),
                pltpu.VMEM((3, 8, points), BF),
                pltpu.VMEM((8, points), BF),
                pltpu.VMEM((1, points), jnp.int32),
                pltpu.VMEM((feats, 2, 8, points), BF),
                pltpu.VMEM((feats, 8, panel), BF),
                pltpu.VMEM((8, feats, 3, 8, panel), BF),
                pltpu.VMEM((256, points), BF),
                pltpu.VMEM((feats * columns, points), F32),
                pltpu.VMEM((feats * columns, points), F32),
                pltpu.VMEM((chunks, feats, 2, 8, points // chunks), BF),
                pltpu.VMEM((chunks, feats, 2, 8, points // chunks), BF),
                pltpu.SemaphoreType.REGULAR,
                dma((5,)),
                dma((feats,)), dma((feats,)), dma((feats,)), dma((feats,)),
                dma((2, feats)), dma((8, feats)), dma((8, feats)),
                dma((chunks, feats)), dma((chunks, feats)),
            ],
            compiler_params=pltpu.CompilerParams(
                collective_id=0, has_side_effects=True, vmem_limit_bytes=16 << 20
            ),
        )(placed(ft), placed(pt), theta, placed(block_mask), placed(order))
        return out_k.T, out_d.T

    return jax.shard_map(
        body,
        mesh=mesh,
        in_specs=(P("rows", "feat"), P("rows", "feat"), P(), P("rows", None), P("rows", None)),
        out_specs=(P("rows", "feat"), P("rows", "feat")),
        check_vma=False,
    )
```

```python
import functools

import jax
import jax.numpy as jnp
from jax import lax
from jax.experimental import pallas as pl
from jax.experimental.pallas import tpu as pltpu
from jax.sharding import PartitionSpec as P

MESH = pl.DeviceIdType.MESH
BF = jnp.bfloat16
F32 = jnp.float32
OFFS = (1, -1, 2, -2, 3, -3, 4, -4)
SLOT = {k: i for i, k in enumerate(OFFS)}
TINY = 1e-30
LATE_GROUPS = ((1, 2), (3,), (4,))
FAR = ((0, -2), (0, -3), (0, -4), (1, -2), (1, -4), (2, -3), (2, -4), (3, -4))
UP = ((1, 1), (1, 2), (1, 3), (1, 4), (3, 3), (3, 4))


def rounded(value):
    return value.astype(BF).astype(F32)


def split3(value):
    high = rounded(value)
    rest = value - high
    middle = rounded(rest)
    return high, middle, rest - middle


def stacked_rows(rows, width):
    index = lax.broadcasted_iota(jnp.int32, (8, width), 0)
    out = jnp.zeros((8, width), F32)
    for place, row in enumerate(rows):
        out = jnp.where(index == place, row, out)
    return out


def kernel(
    blocks, feats, ft, pt, theta, mask_in, order, out,
    mask, own, raw, order_v, full, own_z, slots, right, acc_k, acc_d, out_s, out_r,
    late_in, load_sem, full_send, full_recv, z_send, z_recv, far_sem, up_sem, slot_send, slot_recv, red_send, red_recv,
):
    row = lax.axis_index("rows")
    col = lax.axis_index("feat")
    points = own.shape[2]
    panel = points // feats
    width = panel

    def at(step):
        return lax.rem(row + step + blocks, blocks)

    def device(step, other):
        return (at(step), other)

    def peer(i):
        return lax.rem(col + i, feats)

    loads = [
        pltpu.make_async_copy(order, order_v, load_sem.at[0]),
        pltpu.make_async_copy(pt, raw, load_sem.at[1]),
        pltpu.make_async_copy(ft, own.at[0:2], load_sem.at[2]),
        pltpu.make_async_copy(ft, full.at[col], load_sem.at[3]),
        pltpu.make_async_copy(mask_in, mask, load_sem.at[4]),
    ]
    for load in loads:
        load.start()

    half = blocks // 2
    place = lax.rem(row, half)
    lowest, highest = place == 0, place == half - 1

    barrier = pltpu.get_barrier_semaphore()

    def greet(target):
        pl.semaphore_signal(barrier, inc=1, device_id=target, device_id_type=MESH)

    def greet_block(step):
        for other in range(feats):
            greet(device(step, other))

    for i in range(1, feats):
        greet((row, peer(i)))
    greet_block(-1)
    pl.when(jnp.logical_not(highest))(lambda: greet_block(1))
    for target, k in FAR:
        pl.when(place == target)(functools.partial(greet_block, k))

    def count(condition):
        return condition.astype(jnp.int32)

    greeted = (feats - 1) + feats + feats * count(place != 0)
    for target, k in FAR:
        greeted = greeted + feats * count(place == half + target + k)

    loads[0].wait()
    loads[1].wait()
    wanted = order_v[...]
    ordered = jnp.zeros((8, points), F32)
    for part in range(points // panel):
        source = lax.broadcasted_iota(jnp.int32, (panel, points), 0) + part * panel
        chosen = jnp.where(source == wanted, 1.0, 0.0).astype(BF)
        ordered = ordered + jnp.dot(
            raw[:, part * panel : (part + 1) * panel], chosen, preferred_element_type=F32
        )
    own[2] = ordered.astype(BF)
    for load in loads[2:]:
        load.wait()
    scale16 = 16.0 * jnp.exp(jnp.full((1, panel), -2.0 * theta[0], F32))
    mine = pl.ds(pl.multiple_of(col * panel, panel), panel)
    own_z[col] = own[2, :, mine]

    pl.semaphore_wait(barrier, greeted)

    ups = sorted({below for below, _ in UP})
    for below in ups:
        @pl.when(place == half - below)
        def _():
            for other in range(feats):
                pl.semaphore_signal(late_in, inc=1, device_id=device(below, other), device_id_type=MESH)

    sent = []

    def direct(k, i):
        other = peer(i)
        return pltpu.make_async_remote_copy(
            src_ref=own.at[:, :, pl.ds(pl.multiple_of(other * panel, panel), panel)],
            dst_ref=slots.at[SLOT[k], col],
            send_sem=slot_send.at[SLOT[k], i],
            recv_sem=slot_recv.at[SLOT[k], col],
            device_id=device(-k, other),
            device_id_type=MESH,
        )

    def forward(k, i):
        source = peer(i)
        step = 1 if k > 0 else -1
        return pltpu.make_async_remote_copy(
            src_ref=slots.at[SLOT[k - step], source],
            dst_ref=slots.at[SLOT[k], source],
            send_sem=slot_send.at[SLOT[k], i],
            recv_sem=slot_recv.at[SLOT[k], source],
            device_id=device(-step, col),
            device_id_type=MESH,
        )

    def far_send(target, k, i):
        other = peer(i)
        return pltpu.make_async_remote_copy(
            src_ref=own.at[:, :, pl.ds(pl.multiple_of(other * panel, panel), panel)],
            dst_ref=slots.at[SLOT[k], col],
            send_sem=far_sem.at[target, i],
            recv_sem=slot_recv.at[SLOT[k], col],
            device_id=device(-k, other),
            device_id_type=MESH,
        )

    def up_send(below, k, i):
        other = peer(i)
        if k == below:
            source, lanes = col, pl.ds(pl.multiple_of(other * panel, panel), panel)
            src_ref, target = own.at[:, :, lanes], device(-below, other)
        else:
            source = other
            src_ref, target = slots.at[SLOT[k - below], other], device(-below, col)
        return pltpu.make_async_remote_copy(
            src_ref=src_ref,
            dst_ref=slots.at[SLOT[k], source],
            send_sem=up_sem.at[UP.index((below, k)), i],
            recv_sem=slot_recv.at[SLOT[k], source],
            device_id=target,
            device_id_type=MESH,
        )

    def start_all(make, *which):
        for i in range(feats):
            make(*which, i).start()

    def wait_all(make, *which):
        for i in range(feats):
            make(*which, i).wait_send()

    def forwarded(k):
        if k > 0:
            far = [0] + [half - below + 1 for below, slot in UP if slot == k and below > 1]
        else:
            far = [half - 1] + [target - 1 for target, slot in FAR if slot == k and target > 0]
        yes = place != far[0]
        for other in far[1:]:
            yes = yes & (place != other)
        return yes

    pl.when(highest)(functools.partial(start_all, direct, -1))
    for target, k in FAR:
        pl.when(place == half + target + k)(functools.partial(start_all, far_send, target, k))
    pl.when(jnp.logical_not(highest))(functools.partial(start_all, direct, -1))
    pl.when(jnp.logical_not(lowest))(functools.partial(start_all, direct, 1))
    for i in range(1, feats):
        other = peer(i)
        copy = pltpu.make_async_remote_copy(
            src_ref=own.at[0:2],
            dst_ref=full.at[col],
            send_sem=full_send.at[i],
            recv_sem=full_recv.at[col],
            device_id=(row, other),
            device_id_type=MESH,
        )
        copy.start()
        sent.append(copy)
        copy = pltpu.make_async_remote_copy(
            src_ref=own.at[2, :, pl.ds(pl.multiple_of(other * panel, panel), panel)],
            dst_ref=own_z.at[col],
            send_sem=z_send.at[i],
            recv_sem=z_recv.at[col],
            device_id=(row, other),
            device_id_type=MESH,
        )
        copy.start()
        sent.append(copy)

    def arrival(k, source):
        return pltpu.make_async_remote_copy(
            src_ref=slots.at[SLOT[k], source],
            dst_ref=slots.at[SLOT[k], source],
            send_sem=slot_send.at[SLOT[k], 0],
            recv_sem=slot_recv.at[SLOT[k], source],
            device_id=(row, peer(1)),
            device_id_type=MESH,
        )

    def wait_and_forward(k):
        further = k + (1 if k > 0 else -1)
        for i in range(feats):
            arrival(k, peer(i)).wait_recv()
            if abs(further) <= 4:
                pl.when(forwarded(further))(forward(further, i).start)

    def panel_left(feature_rows):
        squares = jnp.sum(feature_rows * feature_rows, axis=0, keepdims=True) * scale16
        packed = feature_rows.astype(BF)
        one = jnp.ones((1, panel), F32)
        extra = stacked_rows([*split3(squares), one, one, one], panel)
        extra = jnp.concatenate([extra, jnp.zeros((56, panel), F32)], axis=0).astype(BF)
        flat = jnp.concatenate([packed, packed, packed, extra], axis=0)
        return flat.T

    acc_k[...] = jnp.zeros_like(acc_k)
    acc_d[...] = jnp.zeros_like(acc_d)

    def tile(left, z, c):
        lanes = pl.ds(c * width, width)
        x = jnp.dot(left, right[:, lanes], preferred_element_type=F32)
        x = jnp.maximum(x, TINY)
        r = x * lax.rsqrt(x)
        u = jnp.maximum(4.0 - r, 0.0)
        u3 = u * u * u
        kern = (u3 * (u * (r + 1.0))).astype(BF)
        deriv = (u3 * (1.25 * x)).astype(BF)
        return (
            jnp.dot(z, kern, preferred_element_type=F32),
            jnp.dot(z, deriv, preferred_element_type=F32),
        )

    upper = count(place >= half // 2)

    def slot_operands(k):
        near = upper if k > 0 else 1 - upper
        values = slots[2 * (abs(k) - 1) + near].astype(F32)
        features = values[:, 0:2].reshape(64, panel)
        active = jnp.where(mask[0, 4 + abs(k) * (1 - 2 * near)] > 0, 1.0, 0.0)
        z = (values[:, 2].reshape(32, panel) * active).astype(BF)
        return panel_left(features), z

    def take(k):
        pl.when(place + k < half)(functools.partial(wait_and_forward, k))
        pl.when(place >= k)(functools.partial(wait_and_forward, -k))

    take(1)
    for i in range(1, feats):
        source = peer(i)
        pltpu.make_async_remote_copy(
            src_ref=own.at[0:2], dst_ref=full.at[source], send_sem=full_send.at[i],
            recv_sem=full_recv.at[source], device_id=(row, source), device_id_type=MESH,
        ).wait_recv()
        pltpu.make_async_remote_copy(
            src_ref=own_z.at[source], dst_ref=own_z.at[source], send_sem=z_send.at[i],
            recv_sem=z_recv.at[source], device_id=(row, source), device_id_type=MESH,
        ).wait_recv()

    for c in range(points // width):
        lanes = slice(c * width, (c + 1) * width)
        f = full[:, :, :, lanes].astype(F32).reshape(64, width)
        squares = jnp.sum(f * f, axis=0, keepdims=True) * scale16
        one = jnp.ones((1, width), F32)
        extra = stacked_rows([one, one, one, *split3(squares)], width)
        extra = jnp.concatenate([extra, jnp.zeros((56, width), F32)], axis=0)
        high, middle, low = split3(f * (-2.0 * scale16))
        right[:, lanes] = jnp.concatenate([high, middle, low, extra], axis=0).astype(BF)

    def accumulate(pairs):
        for c in range(points // width):
            lanes = pl.ds(c * width, width)
            total_k, total_d = acc_k[:, lanes], acc_d[:, lanes]
            for left, z in pairs:
                add_k, add_d = tile(left, z, c)
                total_k, total_d = total_k + add_k, total_d + add_d
            acc_k[:, lanes], acc_d[:, lanes] = total_k, total_d

    own_features = full[:, :, :, mine].astype(F32).reshape(64, panel)
    own_probes = own_z[...].astype(F32).reshape(32, panel).astype(BF)
    accumulate([(panel_left(own_features), own_probes)])

    accumulate([slot_operands(1)])
    for k in (2, 3, 4):
        take(k)
        accumulate([slot_operands(k)])

    @pl.when(lowest)
    def _():
        pl.semaphore_wait(late_in, feats * len(ups))
        for below, k in UP:
            start_all(up_send, below, k)

    def take_late(k):
        pl.when(place + k >= half)(functools.partial(wait_and_forward, k))
        pl.when(place < k)(functools.partial(wait_and_forward, -k))

    for group in LATE_GROUPS:
        for k in group:
            take_late(k)
        if 4 not in group:
            accumulate([slot_operands(-k) for k in group])
    last = [slot_operands(-4)]
    for c in range(points // width):
        lanes = pl.ds(c * width, width)
        total_k, total_d = acc_k[:, lanes], acc_d[:, lanes]
        for left, z in last:
            add_k, add_d = tile(left, z, c)
            total_k, total_d = total_k + add_k, total_d + add_d
        total_k, total_d = total_k * (1.0 / 256.0), total_d * (1.0 / 64.0)
        acc_k[:, lanes], acc_d[:, lanes] = total_k, total_d
        out_s[c, :, 0] = total_k.astype(BF).reshape(feats, 8, width)
        out_s[c, :, 1] = total_d.astype(BF).reshape(feats, 8, width)
        for i in range(1, feats):
            other = peer(i)
            copy = pltpu.make_async_remote_copy(
                src_ref=out_s.at[c, other],
                dst_ref=out_r.at[c, col],
                send_sem=red_send.at[c, i],
                recv_sem=red_recv.at[c, col],
                device_id=(row, other),
                device_id_type=MESH,
            )
            copy.start()
            sent.append(copy)

    probes_here = pl.ds(pl.multiple_of(col * 8, 8), 8)
    for c in range(points // width):
        lanes = pl.ds(c * width, width)
        total_k, total_d = acc_k[probes_here, lanes], acc_d[probes_here, lanes]
        for i in range(1, feats):
            source = peer(i)
            pltpu.make_async_remote_copy(
                src_ref=out_s.at[c, source], dst_ref=out_r.at[c, source], send_sem=red_send.at[c, i],
                recv_sem=red_recv.at[c, source], device_id=(row, source), device_id_type=MESH,
            ).wait_recv()
            total_k = total_k + out_r[c, source, 0].astype(F32)
            total_d = total_d + out_r[c, source, 1].astype(F32)
        out[0, :, lanes], out[1, :, lanes] = total_k, total_d

    for copy in sent:
        copy.wait_send()
    wait_all(direct, -1)
    pl.when(jnp.logical_not(lowest))(functools.partial(wait_all, direct, 1))
    for k in (2, 3, 4, -2, -3, -4):
        pl.when(forwarded(k))(functools.partial(wait_all, forward, k))

    @pl.when(lowest)
    def _():
        for below, k in UP:
            wait_all(up_send, below, k)

    for target, k in FAR:
        pl.when(place == half + target + k)(functools.partial(wait_all, far_send, target, k))


def solution(mesh):
    blocks, feats = mesh.shape["rows"], mesh.shape["feat"]

    def body(features, probes, theta, block_mask, order):
        points, width = features.shape
        columns = probes.shape[1]
        panel = points // feats
        chunks = feats
        ft = features.T.reshape(2, width // 2, points)
        pt = probes.T
        hbm = pl.BlockSpec(memory_space=pltpu.HBM)
        small = pl.BlockSpec(memory_space=pltpu.SMEM)
        placed = functools.partial(pltpu.with_memory_space_constraint, memory_space=pltpu.HBM)
        vmem = pl.BlockSpec(memory_space=pltpu.VMEM)
        dma = pltpu.SemaphoreType.DMA
        out = pl.pallas_call(
            functools.partial(kernel, blocks, feats),
            out_shape=jax.ShapeDtypeStruct((2, columns, points), F32),
            in_specs=[hbm, hbm, small, hbm, hbm],
            out_specs=vmem,
            scratch_shapes=[
                pltpu.SMEM((1, block_mask.shape[1]), jnp.int32),
                pltpu.VMEM((3, 8, points), BF),
                pltpu.VMEM((8, points), BF),
                pltpu.VMEM((1, points), jnp.int32),
                pltpu.VMEM((feats, 2, 8, points), BF),
                pltpu.VMEM((feats, 8, panel), BF),
                pltpu.VMEM((8, feats, 3, 8, panel), BF),
                pltpu.VMEM((256, points), BF),
                pltpu.VMEM((feats * columns, points), F32),
                pltpu.VMEM((feats * columns, points), F32),
                pltpu.VMEM((chunks, feats, 2, 8, points // chunks), BF),
                pltpu.VMEM((chunks, feats, 2, 8, points // chunks), BF),
                pltpu.SemaphoreType.REGULAR,
                dma((5,)),
                dma((feats,)), dma((feats,)), dma((feats,)), dma((feats,)),
                dma((4, feats)), dma((len(UP), feats)), dma((8, feats)), dma((8, feats)),
                dma((chunks, feats)), dma((chunks, feats)),
            ],
            compiler_params=pltpu.CompilerParams(
                collective_id=0, has_side_effects=True, vmem_limit_bytes=16 << 20
            ),
        )(placed(ft), placed(pt), theta, placed(block_mask), placed(order))
        return out[0].T, out[1].T

    return jax.shard_map(
        body,
        mesh=mesh,
        in_specs=(P("rows", "feat"), P("rows", "feat"), P(), P("rows", None), P("rows", None)),
        out_specs=(P("rows", "feat"), P("rows", "feat")),
        check_vma=False,
    )
```

```python
import functools

import jax
import jax.numpy as jnp
from jax import lax
from jax.experimental import pallas as pl
from jax.experimental.pallas import tpu as pltpu
from jax.sharding import PartitionSpec as P

MESH = pl.DeviceIdType.MESH
BF = jnp.bfloat16
F32 = jnp.float32
OFFS = (1, -1, 2, -2, 3, -3, 4, -4)
SLOT = {k: i for i, k in enumerate(OFFS)}
TINY = 1e-30
LATE_GROUPS = ((1, 2), (3, 4))
FAR = ((0, -2), (0, -4), (1, -2), (1, -4), (2, -4), (3, -4))
BACK = ((0, -3), (1, -3), (2, -3))
GREETED = (*FAR, (0, -3))
UP = ((1, 1), (1, 2), (1, 3), (1, 4), (3, 3), (3, 4))


def rounded(value):
    return value.astype(BF).astype(F32)


def split3(value):
    high = rounded(value)
    rest = value - high
    middle = rounded(rest)
    return high, middle, rest - middle


def stacked_rows(rows, width):
    index = lax.broadcasted_iota(jnp.int32, (8, width), 0)
    out = jnp.zeros((8, width), F32)
    for place, row in enumerate(rows):
        out = jnp.where(index == place, row, out)
    return out


def kernel(
    blocks, feats, ft, pt, theta, mask_in, order, out,
    mask, own, raw, order_v, full, own_z, slots, right, acc_k, acc_d, out_s, out_r,
    late_in, load_sem, full_send, full_recv, z_send, z_recv, far_sem, back_sem, up_sem, slot_send, slot_recv, red_send, red_recv,
):
    row = lax.axis_index("rows")
    col = lax.axis_index("feat")
    points = own.shape[2]
    panel = points // feats
    width = panel

    def at(step):
        return lax.rem(row + step + blocks, blocks)

    def device(step, other):
        return (at(step), other)

    def peer(i):
        return lax.rem(col + i, feats)

    loads = [
        pltpu.make_async_copy(order, order_v, load_sem.at[0]),
        pltpu.make_async_copy(pt, raw, load_sem.at[1]),
        pltpu.make_async_copy(ft, own.at[0:2], load_sem.at[2]),
        pltpu.make_async_copy(ft, full.at[col], load_sem.at[3]),
        pltpu.make_async_copy(mask_in, mask, load_sem.at[4]),
    ]
    for load in loads:
        load.start()

    half = blocks // 2
    place = lax.rem(row, half)
    lowest, highest = place == 0, place == half - 1

    barrier = pltpu.get_barrier_semaphore()

    def greet(target):
        pl.semaphore_signal(barrier, inc=1, device_id=target, device_id_type=MESH)

    def greet_block(step):
        for other in range(feats):
            greet(device(step, other))

    for i in range(1, feats):
        greet((row, peer(i)))
    greet_block(-1)
    pl.when(jnp.logical_not(highest))(lambda: greet_block(1))
    for target, k in GREETED:
        pl.when(place == target)(functools.partial(greet_block, k))

    def count(condition):
        return condition.astype(jnp.int32)

    greeted = (feats - 1) + feats + feats * count(place != 0)
    for target, k in GREETED:
        greeted = greeted + feats * count(place == half + target + k)

    loads[0].wait()
    loads[1].wait()
    wanted = order_v[...]
    ordered = jnp.zeros((8, points), F32)
    for part in range(points // panel):
        source = lax.broadcasted_iota(jnp.int32, (panel, points), 0) + part * panel
        chosen = jnp.where(source == wanted, 1.0, 0.0).astype(BF)
        ordered = ordered + jnp.dot(
            raw[:, part * panel : (part + 1) * panel], chosen, preferred_element_type=F32
        )
    own[2] = ordered.astype(BF)
    for load in loads[2:]:
        load.wait()
    scale16 = 16.0 * jnp.exp(jnp.full((1, panel), -2.0 * theta[0], F32))
    mine = pl.ds(pl.multiple_of(col * panel, panel), panel)
    own_z[col] = own[2, :, mine]

    pl.semaphore_wait(barrier, greeted)

    ups = sorted({below for below, _ in UP})
    for below in ups:
        @pl.when(place == half - below)
        def _():
            for other in range(feats):
                pl.semaphore_signal(late_in, inc=1, device_id=device(below, other), device_id_type=MESH)

    sent = []

    def direct(k, i):
        other = peer(i)
        return pltpu.make_async_remote_copy(
            src_ref=own.at[:, :, pl.ds(pl.multiple_of(other * panel, panel), panel)],
            dst_ref=slots.at[SLOT[k], col],
            send_sem=slot_send.at[SLOT[k], i],
            recv_sem=slot_recv.at[SLOT[k], col],
            device_id=device(-k, other),
            device_id_type=MESH,
        )

    def forward(k, i):
        source = peer(i)
        step = 1 if k > 0 else -1
        return pltpu.make_async_remote_copy(
            src_ref=slots.at[SLOT[k - step], source],
            dst_ref=slots.at[SLOT[k], source],
            send_sem=slot_send.at[SLOT[k], i],
            recv_sem=slot_recv.at[SLOT[k], source],
            device_id=device(-step, col),
            device_id_type=MESH,
        )

    def far_send(target, k, i):
        other = peer(i)
        return pltpu.make_async_remote_copy(
            src_ref=own.at[:, :, pl.ds(pl.multiple_of(other * panel, panel), panel)],
            dst_ref=slots.at[SLOT[k], col],
            send_sem=far_sem.at[target, i],
            recv_sem=slot_recv.at[SLOT[k], col],
            device_id=device(-k, other),
            device_id_type=MESH,
        )

    def up_send(below, k, i):
        other = peer(i)
        if k == below:
            source, lanes = col, pl.ds(pl.multiple_of(other * panel, panel), panel)
            src_ref, target = own.at[:, :, lanes], device(-below, other)
        else:
            source = other
            src_ref, target = slots.at[SLOT[k - below], other], device(-below, col)
        return pltpu.make_async_remote_copy(
            src_ref=src_ref,
            dst_ref=slots.at[SLOT[k], source],
            send_sem=up_sem.at[UP.index((below, k)), i],
            recv_sem=slot_recv.at[SLOT[k], source],
            device_id=target,
            device_id_type=MESH,
        )

    def back(i):
        source = peer(i)
        return pltpu.make_async_remote_copy(
            src_ref=slots.at[SLOT[-4], source],
            dst_ref=slots.at[SLOT[-3], source],
            send_sem=back_sem.at[i],
            recv_sem=slot_recv.at[SLOT[-3], source],
            device_id=device(-1, col),
            device_id_type=MESH,
        )

    def start_all(make, *which):
        for i in range(feats):
            make(*which, i).start()

    def wait_all(make, *which):
        for i in range(feats):
            make(*which, i).wait_send()

    def forwarded(k):
        if k > 0:
            far = [0] + [half - below + 1 for below, slot in UP if slot == k and below > 1]
        else:
            far = [half - 1] + [target - 1 for target, slot in FAR + BACK if slot == k and target > 0]
        yes = place != far[0]
        for other in far[1:]:
            yes = yes & (place != other)
        return yes

    pl.when(highest)(functools.partial(start_all, direct, -1))
    for target, k in FAR:
        pl.when(place == half + target + k)(functools.partial(start_all, far_send, target, k))
    pl.when(jnp.logical_not(highest))(functools.partial(start_all, direct, -1))
    pl.when(jnp.logical_not(lowest))(functools.partial(start_all, direct, 1))
    for i in range(1, feats):
        other = peer(i)
        copy = pltpu.make_async_remote_copy(
            src_ref=own.at[0:2],
            dst_ref=full.at[col],
            send_sem=full_send.at[i],
            recv_sem=full_recv.at[col],
            device_id=(row, other),
            device_id_type=MESH,
        )
        copy.start()
        sent.append(copy)
        copy = pltpu.make_async_remote_copy(
            src_ref=own.at[2, :, pl.ds(pl.multiple_of(other * panel, panel), panel)],
            dst_ref=own_z.at[col],
            send_sem=z_send.at[i],
            recv_sem=z_recv.at[col],
            device_id=(row, other),
            device_id_type=MESH,
        )
        copy.start()
        sent.append(copy)

    def arrival(k, source):
        return pltpu.make_async_remote_copy(
            src_ref=slots.at[SLOT[k], source],
            dst_ref=slots.at[SLOT[k], source],
            send_sem=slot_send.at[SLOT[k], 0],
            recv_sem=slot_recv.at[SLOT[k], source],
            device_id=(row, peer(1)),
            device_id_type=MESH,
        )

    def wait_and_forward(k):
        further = k + (1 if k > 0 else -1)
        for i in range(feats):
            arrival(k, peer(i)).wait_recv()
            if abs(further) <= 4:
                pl.when(forwarded(further))(forward(further, i).start)

    def panel_left(feature_rows):
        squares = jnp.sum(feature_rows * feature_rows, axis=0, keepdims=True) * scale16
        packed = feature_rows.astype(BF)
        one = jnp.ones((1, panel), F32)
        extra = stacked_rows([*split3(squares), one, one, one], panel)
        extra = jnp.concatenate([extra, jnp.zeros((56, panel), F32)], axis=0).astype(BF)
        flat = jnp.concatenate([packed, packed, packed, extra], axis=0)
        return flat.T

    acc_k[...] = jnp.zeros_like(acc_k)
    acc_d[...] = jnp.zeros_like(acc_d)

    def distances(left, c):
        return jnp.dot(left, right[:, pl.ds(c * width, width)], preferred_element_type=F32)

    def profiles(x):
        x = jnp.maximum(x, TINY)
        r = x * lax.rsqrt(x)
        u = jnp.maximum(4.0 - r, 0.0)
        u3 = u * u * u
        return (u3 * (u * (r + 1.0))).astype(BF), (u3 * (1.25 * x)).astype(BF)

    def products(z, pair):
        return tuple(jnp.dot(z, part, preferred_element_type=F32) for part in pair)

    def tile(left, z, c):
        return products(z, profiles(distances(left, c)))

    upper = count(place >= half // 2)

    def slot_operands(k):
        near = upper if k > 0 else 1 - upper
        values = slots[2 * (abs(k) - 1) + near].astype(F32)
        features = values[:, 0:2].reshape(64, panel)
        active = jnp.where(mask[0, 4 + abs(k) * (1 - 2 * near)] > 0, 1.0, 0.0)
        z = (values[:, 2].reshape(32, panel) * active).astype(BF)
        return panel_left(features), z

    def take(k):
        pl.when(place + k < half)(functools.partial(wait_and_forward, k))
        pl.when(place >= k)(functools.partial(wait_and_forward, -k))

    take(1)
    for i in range(1, feats):
        source = peer(i)
        pltpu.make_async_remote_copy(
            src_ref=own.at[0:2], dst_ref=full.at[source], send_sem=full_send.at[i],
            recv_sem=full_recv.at[source], device_id=(row, source), device_id_type=MESH,
        ).wait_recv()
        pltpu.make_async_remote_copy(
            src_ref=own_z.at[source], dst_ref=own_z.at[source], send_sem=z_send.at[i],
            recv_sem=z_recv.at[source], device_id=(row, source), device_id_type=MESH,
        ).wait_recv()

    for c in range(points // width):
        lanes = slice(c * width, (c + 1) * width)
        f = full[:, :, :, lanes].astype(F32).reshape(64, width)
        squares = jnp.sum(f * f, axis=0, keepdims=True) * scale16
        one = jnp.ones((1, width), F32)
        extra = stacked_rows([one, one, one, *split3(squares)], width)
        extra = jnp.concatenate([extra, jnp.zeros((56, width), F32)], axis=0)
        high, middle, low = split3(f * (-2.0 * scale16))
        right[:, lanes] = jnp.concatenate([high, middle, low, extra], axis=0).astype(BF)

    def accumulate(pairs):
        for c in range(points // width):
            lanes = pl.ds(c * width, width)
            total_k, total_d = acc_k[:, lanes], acc_d[:, lanes]
            for left, z in pairs:
                add_k, add_d = tile(left, z, c)
                total_k, total_d = total_k + add_k, total_d + add_d
            acc_k[:, lanes], acc_d[:, lanes] = total_k, total_d

    own_features = full[:, :, :, mine].astype(F32).reshape(64, panel)
    own_probes = own_z[...].astype(F32).reshape(32, panel).astype(BF)
    accumulate([(panel_left(own_features), own_probes)])

    accumulate([slot_operands(1)])
    for k in (2, 3, 4):
        take(k)
        accumulate([slot_operands(k)])

    @pl.when(lowest)
    def _():
        pl.semaphore_wait(late_in, feats * len(ups))
        for below, k in UP:
            start_all(up_send, below, k)

    @pl.when((place > 0) & (place < 4))
    def _():
        for i in range(feats):
            arrival(-4, peer(i)).wait_recv()
            back(i).start()

    def take_late(k):
        pl.when(place + k >= half)(functools.partial(wait_and_forward, k))
        late = place < k if k < 4 else place == 0
        pl.when(late)(functools.partial(wait_and_forward, -k))

    for group in LATE_GROUPS[:-1]:
        for k in group:
            take_late(k)
        accumulate([slot_operands(-k) for k in group])

    def hand_out(c, parts):
        lanes = pl.ds(c * width, width)
        total_k, total_d = acc_k[:, lanes], acc_d[:, lanes]
        for add_k, add_d in parts:
            total_k, total_d = total_k + add_k, total_d + add_d
        total_k, total_d = total_k * (1.0 / 256.0), total_d * (1.0 / 64.0)
        acc_k[:, lanes], acc_d[:, lanes] = total_k, total_d
        out_s[c, :, 0] = total_k.astype(BF).reshape(feats, 8, width)
        out_s[c, :, 1] = total_d.astype(BF).reshape(feats, 8, width)
        for i in range(1, feats):
            other = peer(i)
            copy = pltpu.make_async_remote_copy(
                src_ref=out_s.at[c, other],
                dst_ref=out_r.at[c, col],
                send_sem=red_send.at[c, i],
                recv_sem=red_recv.at[c, col],
                device_id=(row, other),
                device_id_type=MESH,
            )
            copy.start()
            sent.append(copy)

    for k in LATE_GROUPS[-1]:
        take_late(k)
    last = [slot_operands(-k) for k in LATE_GROUPS[-1]]
    chunks = points // width
    x = {c: [distances(left, c) for left, _ in last] for c in range(min(2, chunks))}
    pairs = [profiles(part) for part in x.pop(0)]
    for c in range(chunks):
        if c + 2 < chunks:
            x[c + 2] = [distances(left, c + 2) for left, _ in last]
        parts = [products(z, pair) for (_, z), pair in zip(last, pairs)]
        if c + 1 < chunks:
            pairs = [profiles(part) for part in x.pop(c + 1)]
        hand_out(c, parts)

    probes_here = pl.ds(pl.multiple_of(col * 8, 8), 8)
    for c in range(points // width):
        lanes = pl.ds(c * width, width)
        total_k, total_d = acc_k[probes_here, lanes], acc_d[probes_here, lanes]
        for i in range(1, feats):
            source = peer(i)
            pltpu.make_async_remote_copy(
                src_ref=out_s.at[c, source], dst_ref=out_r.at[c, source], send_sem=red_send.at[c, i],
                recv_sem=red_recv.at[c, source], device_id=(row, source), device_id_type=MESH,
            ).wait_recv()
            total_k = total_k + out_r[c, source, 0].astype(F32)
            total_d = total_d + out_r[c, source, 1].astype(F32)
        out[0, :, lanes], out[1, :, lanes] = total_k, total_d

    for copy in sent:
        copy.wait_send()
    pl.when((place > 0) & (place < 4))(functools.partial(wait_all, back))
    wait_all(direct, -1)
    pl.when(jnp.logical_not(lowest))(functools.partial(wait_all, direct, 1))
    for k in (2, 3, 4, -2, -3, -4):
        pl.when(forwarded(k))(functools.partial(wait_all, forward, k))

    @pl.when(lowest)
    def _():
        for below, k in UP:
            wait_all(up_send, below, k)

    for target, k in FAR:
        pl.when(place == half + target + k)(functools.partial(wait_all, far_send, target, k))


def solution(mesh):
    blocks, feats = mesh.shape["rows"], mesh.shape["feat"]

    def body(features, probes, theta, block_mask, order):
        points, width = features.shape
        columns = probes.shape[1]
        panel = points // feats
        chunks = feats
        ft = features.T.reshape(2, width // 2, points)
        pt = probes.T
        hbm = pl.BlockSpec(memory_space=pltpu.HBM)
        small = pl.BlockSpec(memory_space=pltpu.SMEM)
        placed = functools.partial(pltpu.with_memory_space_constraint, memory_space=pltpu.HBM)
        vmem = pl.BlockSpec(memory_space=pltpu.VMEM)
        dma = pltpu.SemaphoreType.DMA
        out = pl.pallas_call(
            functools.partial(kernel, blocks, feats),
            out_shape=jax.ShapeDtypeStruct((2, columns, points), F32),
            in_specs=[hbm, hbm, small, hbm, hbm],
            out_specs=vmem,
            scratch_shapes=[
                pltpu.SMEM((1, block_mask.shape[1]), jnp.int32),
                pltpu.VMEM((3, 8, points), BF),
                pltpu.VMEM((8, points), BF),
                pltpu.VMEM((1, points), jnp.int32),
                pltpu.VMEM((feats, 2, 8, points), BF),
                pltpu.VMEM((feats, 8, panel), BF),
                pltpu.VMEM((8, feats, 3, 8, panel), BF),
                pltpu.VMEM((256, points), BF),
                pltpu.VMEM((feats * columns, points), F32),
                pltpu.VMEM((feats * columns, points), F32),
                pltpu.VMEM((chunks, feats, 2, 8, points // chunks), BF),
                pltpu.VMEM((chunks, feats, 2, 8, points // chunks), BF),
                pltpu.SemaphoreType.REGULAR,
                dma((5,)),
                dma((feats,)), dma((feats,)), dma((feats,)), dma((feats,)),
                dma((4, feats)), dma((feats,)), dma((len(UP), feats)), dma((8, feats)), dma((8, feats)),
                dma((chunks, feats)), dma((chunks, feats)),
            ],
            compiler_params=pltpu.CompilerParams(
                collective_id=0, has_side_effects=True, vmem_limit_bytes=16 << 20
            ),
        )(placed(ft), placed(pt), theta, placed(block_mask), placed(order))
        return out[0].T, out[1].T

    return jax.shard_map(
        body,
        mesh=mesh,
        in_specs=(P("rows", "feat"), P("rows", "feat"), P(), P("rows", None), P("rows", None)),
        out_specs=(P("rows", "feat"), P("rows", "feat")),
        check_vma=False,
    )
```

```python
import functools

import jax
import jax.numpy as jnp
from jax import lax
from jax.experimental import pallas as pl
from jax.experimental.pallas import tpu as pltpu
from jax.sharding import PartitionSpec as P

MESH = pl.DeviceIdType.MESH
BF = jnp.bfloat16
F32 = jnp.float32
OFFS = (1, -1, 2, -2, 3, -3, 4, -4)
SLOT = {k: i for i, k in enumerate(OFFS)}
TINY = 1e-30
LATE_GROUPS = ((1, 2), (4, 3))
FAR = ((0, -2), (0, -4), (1, -2), (1, -4), (2, -4), (3, -4))
BACK = ((0, -3), (1, -3), (2, -3))
GREETED = (*FAR, (0, -3))
UP = ((1, 1), (1, 2), (1, 3), (1, 4), (3, 3), (3, 4))


def rounded(value):
    return value.astype(BF).astype(F32)


def split3(value):
    high = rounded(value)
    rest = value - high
    middle = rounded(rest)
    return high, middle, rest - middle


def stacked_rows(rows, width):
    index = lax.broadcasted_iota(jnp.int32, (8, width), 0)
    out = jnp.zeros((8, width), F32)
    for place, row in enumerate(rows):
        out = jnp.where(index == place, row, out)
    return out


def kernel(
    blocks, feats, ft, pt, theta, mask_in, order, out,
    mask, own, raw, order_v, full, own_z, slots, right, acc_k, acc_d, out_s, out_r,
    late_in, load_sem, full_send, full_recv, z_send, z_recv, far_sem, back_sem, up_sem, slot_send, slot_recv, red_send, red_recv,
):
    row = lax.axis_index("rows")
    col = lax.axis_index("feat")
    points = own.shape[2]
    panel = points // feats
    width = panel

    def at(step):
        return lax.rem(row + step + blocks, blocks)

    def device(step, other):
        return (at(step), other)

    def peer(i):
        return lax.rem(col + i, feats)

    loads = [
        pltpu.make_async_copy(order, order_v, load_sem.at[0]),
        pltpu.make_async_copy(pt, raw, load_sem.at[1]),
        pltpu.make_async_copy(ft, own.at[0:2], load_sem.at[2]),
        pltpu.make_async_copy(ft, full.at[col], load_sem.at[3]),
        pltpu.make_async_copy(mask_in, mask, load_sem.at[4]),
    ]
    for load in loads:
        load.start()

    half = blocks // 2
    place = lax.rem(row, half)
    lowest, highest = place == 0, place == half - 1

    barrier = pltpu.get_barrier_semaphore()

    def greet(target):
        pl.semaphore_signal(barrier, inc=1, device_id=target, device_id_type=MESH)

    def greet_block(step):
        for other in range(feats):
            greet(device(step, other))

    for i in range(1, feats):
        greet((row, peer(i)))
    greet_block(-1)
    pl.when(jnp.logical_not(highest))(lambda: greet_block(1))
    for target, k in GREETED:
        pl.when(place == target)(functools.partial(greet_block, k))

    def count(condition):
        return condition.astype(jnp.int32)

    greeted = (feats - 1) + feats + feats * count(place != 0)
    for target, k in GREETED:
        greeted = greeted + feats * count(place == half + target + k)

    loads[0].wait()
    loads[1].wait()
    wanted = order_v[...]
    ordered = jnp.zeros((8, points), F32)
    for part in range(points // panel):
        source = lax.broadcasted_iota(jnp.int32, (panel, points), 0) + part * panel
        chosen = jnp.where(source == wanted, 1.0, 0.0).astype(BF)
        ordered = ordered + jnp.dot(
            raw[:, part * panel : (part + 1) * panel], chosen, preferred_element_type=F32
        )
    own[2] = ordered.astype(BF)
    for load in loads[2:]:
        load.wait()
    scale16 = 16.0 * jnp.exp(jnp.full((1, panel), -2.0 * theta[0], F32))
    mine = pl.ds(pl.multiple_of(col * panel, panel), panel)
    own_z[col] = own[2, :, mine]

    pl.semaphore_wait(barrier, greeted)

    ups = sorted({below for below, _ in UP})
    for below in ups:
        @pl.when(place == half - below)
        def _():
            for other in range(feats):
                pl.semaphore_signal(late_in, inc=1, device_id=device(below, other), device_id_type=MESH)

    sent = []

    def direct(k, i):
        other = peer(i)
        return pltpu.make_async_remote_copy(
            src_ref=own.at[:, :, pl.ds(pl.multiple_of(other * panel, panel), panel)],
            dst_ref=slots.at[SLOT[k], col],
            send_sem=slot_send.at[SLOT[k], i],
            recv_sem=slot_recv.at[SLOT[k], col],
            device_id=device(-k, other),
            device_id_type=MESH,
        )

    def forward(k, i):
        source = peer(i)
        step = 1 if k > 0 else -1
        return pltpu.make_async_remote_copy(
            src_ref=slots.at[SLOT[k - step], source],
            dst_ref=slots.at[SLOT[k], source],
            send_sem=slot_send.at[SLOT[k], i],
            recv_sem=slot_recv.at[SLOT[k], source],
            device_id=device(-step, col),
            device_id_type=MESH,
        )

    def far_send(target, k, i):
        other = peer(i)
        return pltpu.make_async_remote_copy(
            src_ref=own.at[:, :, pl.ds(pl.multiple_of(other * panel, panel), panel)],
            dst_ref=slots.at[SLOT[k], col],
            send_sem=far_sem.at[target, i],
            recv_sem=slot_recv.at[SLOT[k], col],
            device_id=device(-k, other),
            device_id_type=MESH,
        )

    def up_send(below, k, i):
        other = peer(i)
        if k == below:
            source, lanes = col, pl.ds(pl.multiple_of(other * panel, panel), panel)
            src_ref, target = own.at[:, :, lanes], device(-below, other)
        else:
            source = other
            src_ref, target = slots.at[SLOT[k - below], other], device(-below, col)
        return pltpu.make_async_remote_copy(
            src_ref=src_ref,
            dst_ref=slots.at[SLOT[k], source],
            send_sem=up_sem.at[UP.index((below, k)), i],
            recv_sem=slot_recv.at[SLOT[k], source],
            device_id=target,
            device_id_type=MESH,
        )

    def back(i):
        source = peer(i)
        return pltpu.make_async_remote_copy(
            src_ref=slots.at[SLOT[-4], source],
            dst_ref=slots.at[SLOT[-3], source],
            send_sem=back_sem.at[i],
            recv_sem=slot_recv.at[SLOT[-3], source],
            device_id=device(-1, col),
            device_id_type=MESH,
        )

    def start_all(make, *which):
        for i in range(feats):
            make(*which, i).start()

    def wait_all(make, *which):
        for i in range(feats):
            make(*which, i).wait_send()

    def forwarded(k):
        if k > 0:
            far = [0] + [half - below + 1 for below, slot in UP if slot == k and below > 1]
        else:
            far = [half - 1] + [target - 1 for target, slot in FAR + BACK if slot == k and target > 0]
        yes = place != far[0]
        for other in far[1:]:
            yes = yes & (place != other)
        return yes

    pl.when(highest)(functools.partial(start_all, direct, -1))
    for target, k in FAR:
        pl.when(place == half + target + k)(functools.partial(start_all, far_send, target, k))
    pl.when(jnp.logical_not(highest))(functools.partial(start_all, direct, -1))
    pl.when(jnp.logical_not(lowest))(functools.partial(start_all, direct, 1))
    for i in range(1, feats):
        other = peer(i)
        copy = pltpu.make_async_remote_copy(
            src_ref=own.at[0:2],
            dst_ref=full.at[col],
            send_sem=full_send.at[i],
            recv_sem=full_recv.at[col],
            device_id=(row, other),
            device_id_type=MESH,
        )
        copy.start()
        sent.append(copy)
        copy = pltpu.make_async_remote_copy(
            src_ref=own.at[2, :, pl.ds(pl.multiple_of(other * panel, panel), panel)],
            dst_ref=own_z.at[col],
            send_sem=z_send.at[i],
            recv_sem=z_recv.at[col],
            device_id=(row, other),
            device_id_type=MESH,
        )
        copy.start()
        sent.append(copy)

    def arrival(k, source):
        return pltpu.make_async_remote_copy(
            src_ref=slots.at[SLOT[k], source],
            dst_ref=slots.at[SLOT[k], source],
            send_sem=slot_send.at[SLOT[k], 0],
            recv_sem=slot_recv.at[SLOT[k], source],
            device_id=(row, peer(1)),
            device_id_type=MESH,
        )

    def wait_and_forward(k):
        further = k + (1 if k > 0 else -1)
        for i in range(feats):
            arrival(k, peer(i)).wait_recv()
            if abs(further) <= 4:
                pl.when(forwarded(further))(forward(further, i).start)

    def panel_left(feature_rows):
        squares = jnp.sum(feature_rows * feature_rows, axis=0, keepdims=True) * scale16
        packed = feature_rows.astype(BF)
        one = jnp.ones((1, panel), F32)
        extra = stacked_rows([*split3(squares), one, one, one], panel)
        extra = jnp.concatenate([extra, jnp.zeros((56, panel), F32)], axis=0).astype(BF)
        flat = jnp.concatenate([packed, packed, packed, extra], axis=0)
        return flat.T

    acc_k[...] = jnp.zeros_like(acc_k)
    acc_d[...] = jnp.zeros_like(acc_d)

    def distances(left, c):
        return jnp.dot(left, right[:, pl.ds(c * width, width)], preferred_element_type=F32)

    def profiles(x):
        x = jnp.maximum(x, TINY)
        r = x * lax.rsqrt(x)
        u = jnp.maximum(4.0 - r, 0.0)
        u3 = u * u * u
        return (u3 * (u * (r + 1.0))).astype(BF), (u3 * (1.25 * x)).astype(BF)

    def products(z, pair):
        return tuple(jnp.dot(z, part, preferred_element_type=F32) for part in pair)

    def tile(left, z, c):
        return products(z, profiles(distances(left, c)))

    upper = count(place >= half // 2)

    def slot_operands(k):
        near = upper if k > 0 else 1 - upper
        values = slots[2 * (abs(k) - 1) + near].astype(F32)
        features = values[:, 0:2].reshape(64, panel)
        active = jnp.where(mask[0, 4 + abs(k) * (1 - 2 * near)] > 0, 1.0, 0.0)
        z = (values[:, 2].reshape(32, panel) * active).astype(BF)
        return panel_left(features), z

    def take(k):
        pl.when(place + k < half)(functools.partial(wait_and_forward, k))
        pl.when(place >= k)(functools.partial(wait_and_forward, -k))

    take(1)
    for i in range(1, feats):
        source = peer(i)
        pltpu.make_async_remote_copy(
            src_ref=own.at[0:2], dst_ref=full.at[source], send_sem=full_send.at[i],
            recv_sem=full_recv.at[source], device_id=(row, source), device_id_type=MESH,
        ).wait_recv()
        pltpu.make_async_remote_copy(
            src_ref=own_z.at[source], dst_ref=own_z.at[source], send_sem=z_send.at[i],
            recv_sem=z_recv.at[source], device_id=(row, source), device_id_type=MESH,
        ).wait_recv()

    for c in range(points // width):
        lanes = slice(c * width, (c + 1) * width)
        f = full[:, :, :, lanes].astype(F32).reshape(64, width)
        squares = jnp.sum(f * f, axis=0, keepdims=True) * scale16
        one = jnp.ones((1, width), F32)
        extra = stacked_rows([one, one, one, *split3(squares)], width)
        extra = jnp.concatenate([extra, jnp.zeros((56, width), F32)], axis=0)
        high, middle, low = split3(f * (-2.0 * scale16))
        right[:, lanes] = jnp.concatenate([high, middle, low, extra], axis=0).astype(BF)

    def accumulate(pairs):
        for c in range(points // width):
            lanes = pl.ds(c * width, width)
            total_k, total_d = acc_k[:, lanes], acc_d[:, lanes]
            for left, z in pairs:
                add_k, add_d = tile(left, z, c)
                total_k, total_d = total_k + add_k, total_d + add_d
            acc_k[:, lanes], acc_d[:, lanes] = total_k, total_d

    own_features = full[:, :, :, mine].astype(F32).reshape(64, panel)
    own_probes = own_z[...].astype(F32).reshape(32, panel).astype(BF)
    accumulate([(panel_left(own_features), own_probes)])

    accumulate([slot_operands(1)])
    for k in (2, 3, 4):
        take(k)
        accumulate([slot_operands(k)])

    @pl.when(lowest)
    def _():
        pl.semaphore_wait(late_in, feats * len(ups))
        for below, k in UP:
            start_all(up_send, below, k)

    @pl.when((place > 0) & (place < 4))
    def _():
        for i in range(feats):
            arrival(-4, peer(i)).wait_recv()
            back(i).start()

    def take_late(k):
        pl.when(place + k >= half)(functools.partial(wait_and_forward, k))
        late = place < k if k < 4 else place == 0
        pl.when(late)(functools.partial(wait_and_forward, -k))

    for group in LATE_GROUPS[:-1]:
        for k in group:
            take_late(k)
        accumulate([slot_operands(-k) for k in group])

    def hand_out(c, parts):
        lanes = pl.ds(c * width, width)
        total_k, total_d = acc_k[:, lanes], acc_d[:, lanes]
        for add_k, add_d in parts:
            total_k, total_d = total_k + add_k, total_d + add_d
        total_k, total_d = total_k * (1.0 / 256.0), total_d * (1.0 / 64.0)
        acc_k[:, lanes], acc_d[:, lanes] = total_k, total_d
        out_s[c, :, 0] = total_k.astype(BF).reshape(feats, 8, width)
        out_s[c, :, 1] = total_d.astype(BF).reshape(feats, 8, width)
        for i in range(1, feats):
            other = peer(i)
            copy = pltpu.make_async_remote_copy(
                src_ref=out_s.at[c, other],
                dst_ref=out_r.at[c, col],
                send_sem=red_send.at[c, i],
                recv_sem=red_recv.at[c, col],
                device_id=(row, other),
                device_id_type=MESH,
            )
            copy.start()
            sent.append(copy)

    chunks = points // width
    last, x = [], {c: [] for c in range(min(2, chunks))}
    for k in LATE_GROUPS[-1]:
        take_late(k)
        last.append(slot_operands(-k))
        for c in x:
            x[c].append(distances(last[-1][0], c))
    pairs = [profiles(part) for part in x.pop(0)]
    for c in range(chunks):
        if c + 2 < chunks:
            x[c + 2] = [distances(left, c + 2) for left, _ in last]
        parts = [products(z, pair) for (_, z), pair in zip(last, pairs)]
        if c + 1 < chunks:
            pairs = [profiles(part) for part in x.pop(c + 1)]
        hand_out(c, parts)

    probes_here = pl.ds(pl.multiple_of(col * 8, 8), 8)
    for c in range(points // width):
        lanes = pl.ds(c * width, width)
        total_k, total_d = acc_k[probes_here, lanes], acc_d[probes_here, lanes]
        for i in range(1, feats):
            source = peer(i)
            pltpu.make_async_remote_copy(
                src_ref=out_s.at[c, source], dst_ref=out_r.at[c, source], send_sem=red_send.at[c, i],
                recv_sem=red_recv.at[c, source], device_id=(row, source), device_id_type=MESH,
            ).wait_recv()
            total_k = total_k + out_r[c, source, 0].astype(F32)
            total_d = total_d + out_r[c, source, 1].astype(F32)
        out[0, :, lanes], out[1, :, lanes] = total_k, total_d

    for copy in sent:
        copy.wait_send()
    pl.when((place > 0) & (place < 4))(functools.partial(wait_all, back))
    wait_all(direct, -1)
    pl.when(jnp.logical_not(lowest))(functools.partial(wait_all, direct, 1))
    for k in (2, 3, 4, -2, -3, -4):
        pl.when(forwarded(k))(functools.partial(wait_all, forward, k))

    @pl.when(lowest)
    def _():
        for below, k in UP:
            wait_all(up_send, below, k)

    for target, k in FAR:
        pl.when(place == half + target + k)(functools.partial(wait_all, far_send, target, k))


def solution(mesh):
    blocks, feats = mesh.shape["rows"], mesh.shape["feat"]

    def body(features, probes, theta, block_mask, order):
        points, width = features.shape
        columns = probes.shape[1]
        panel = points // feats
        chunks = feats
        ft = features.T.reshape(2, width // 2, points)
        pt = probes.T
        hbm = pl.BlockSpec(memory_space=pltpu.HBM)
        small = pl.BlockSpec(memory_space=pltpu.SMEM)
        placed = functools.partial(pltpu.with_memory_space_constraint, memory_space=pltpu.HBM)
        vmem = pl.BlockSpec(memory_space=pltpu.VMEM)
        dma = pltpu.SemaphoreType.DMA
        out = pl.pallas_call(
            functools.partial(kernel, blocks, feats),
            out_shape=jax.ShapeDtypeStruct((2, columns, points), F32),
            in_specs=[hbm, hbm, small, hbm, hbm],
            out_specs=vmem,
            scratch_shapes=[
                pltpu.SMEM((1, block_mask.shape[1]), jnp.int32),
                pltpu.VMEM((3, 8, points), BF),
                pltpu.VMEM((8, points), BF),
                pltpu.VMEM((1, points), jnp.int32),
                pltpu.VMEM((feats, 2, 8, points), BF),
                pltpu.VMEM((feats, 8, panel), BF),
                pltpu.VMEM((8, feats, 3, 8, panel), BF),
                pltpu.VMEM((256, points), BF),
                pltpu.VMEM((feats * columns, points), F32),
                pltpu.VMEM((feats * columns, points), F32),
                pltpu.VMEM((chunks, feats, 2, 8, points // chunks), BF),
                pltpu.VMEM((chunks, feats, 2, 8, points // chunks), BF),
                pltpu.SemaphoreType.REGULAR,
                dma((5,)),
                dma((feats,)), dma((feats,)), dma((feats,)), dma((feats,)),
                dma((4, feats)), dma((feats,)), dma((len(UP), feats)), dma((8, feats)), dma((8, feats)),
                dma((chunks, feats)), dma((chunks, feats)),
            ],
            compiler_params=pltpu.CompilerParams(
                collective_id=0, has_side_effects=True, vmem_limit_bytes=16 << 20
            ),
        )(placed(ft), placed(pt), theta, placed(block_mask), placed(order))
        return out[0].T, out[1].T

    return jax.shard_map(
        body,
        mesh=mesh,
        in_specs=(P("rows", "feat"), P("rows", "feat"), P(), P("rows", None), P("rows", None)),
        out_specs=(P("rows", "feat"), P("rows", "feat")),
        check_vma=False,
    )
```
